32 devices in a mesh: row: 4 (over y, x), col: 8 (over z, core).
Axes of the slice: x: 2, y: 2, z: 4, core: 2. Of those that a mesh axis runs over, the one named last changes fastest.
Arguments:
- eigenbasis: bfloat16 [16384, 16384], P('row', 'col'), may hold values from -0.046875 to 0.046875
- gradient: float32 [16384, 2048], P('row', 'col'), may hold values from -6 to 6
- moment_one: float32 [16384, 2048], P('col', 'row'), may hold values from -0.6 to 0.6
- moment_two: float32 [16384, 2048], P('col', 'row'), may hold values from 0.0001 to 0.01
Outputs:
- update: float32 [16384, 2048], P('row', 'col')
- new_one: float32 [16384, 2048], P('col', 'row')
- new_two: float32 [16384, 2048], P('col', 'row')
The draws below stay inside these ranges and needn't reach their ends.
All inputs are finite; a program needn't handle non-finite values.
Results may differ from the reference program's by a relative error of at most 0.004.
Values may be sent and summed in bfloat16 or wider, within the bound.
A program may use at most 128 MiB of HBM per device.

```python
import math
import jax
import jax.numpy as jnp

D = 16384
COLS = 2048


def spiked(entries, own_key, source, target, parts, factor):
    owner, partner = [(jnp.arange(entries.shape[position]) // (entries.shape[position] // parts)).reshape([-1 if axis == position else 1 for axis in range(entries.ndim)]) for position in (source, target)]
    chosen = jax.random.permutation(own_key, parts)[partner]
    strong = (owner == chosen) | (owner == (partner + parts // 2) % parts)
    return jnp.where(strong, factor * entries, entries)


def block_scale(own_key, extent, split, low, high):
    def one(position, blocks):
        heights = jax.random.uniform(jax.random.fold_in(jax.random.fold_in(own_key, 6), position), (blocks,), jnp.float32, low / len(split), high / len(split))
        return jnp.repeat(jnp.exp(heights), extent[position] // blocks).reshape((-1,) + (1,) * (len(extent) - position - 1))

    level = one(*split[0])
    for cut in split[1:]:
        level = level * one(*cut)
    return level


def scatter_about(own_key, dims, scale, reach, split=(), dtype=jnp.bfloat16):
    loudness = block_scale(own_key, dims, split, -0.22, 0.18) if split else 1.0
    array = jax.random.normal(own_key, dims, jnp.float32) * scale * loudness
    return jnp.minimum(jnp.maximum(array, -reach), reach).astype(dtype)


def heavy_noise(key, extent, width, limit, split, heavy, held_as=jnp.bfloat16):
    result = width * jax.random.normal(key, extent, jnp.float32)
    if split:
        result = result * block_scale(key, extent, split, -0.22, 0.18)
    return jnp.clip(spiked(result, jax.random.fold_in(key, 3), *heavy), -limit, limit).astype(held_as)


def setup_inputs(seed: int = 0) -> dict:
    key_of = jax.random.split(jax.random.key(seed), 5)
    return {
        "eigenbasis": scatter_about(key_of[0], (D, D), D ** -0.5, 0.046875, ((0, 4), (1, 8))),
        "gradient": heavy_noise(key_of[1], (D, COLS), 1.0, 6.0, ((0, 4), (1, 8)), (0, 1, 8, 2.0), jnp.float32),
        "moment_one": scatter_about(key_of[2], (D, COLS), 0.1, 0.6, ((0, 8), (1, 4)), jnp.float32),
        "moment_two": jnp.clip(jnp.exp(math.log(0.01) - 4.6051702 * jax.random.uniform(key_of[3], (D, COLS), jnp.float32) ** block_scale(key_of[3], (D, COLS), ((0, 8), (1, 4)), -0.2, 0.2)), 0.0001, 0.01),
    }


beta_one = 0.9
beta_two = 0.999
step_count = 10
epsilon = 1e-08

def reference(eigenbasis, gradient, moment_one, moment_two):
    grad_half = gradient.astype(jnp.bfloat16)
    rotated = jnp.dot(eigenbasis.T, grad_half, preferred_element_type=jnp.float32)
    new_one = beta_one * moment_one + (1.0 - beta_one) * rotated
    new_two = beta_two * moment_two + (1.0 - beta_two) * rotated * rotated
    corr_one = 1.0 - beta_one ** step_count
    corr_two = 1.0 - beta_two ** step_count
    direction = (new_one / corr_one / (jnp.sqrt(new_two / corr_two) + epsilon)).astype(jnp.bfloat16)
    update = jnp.dot(eigenbasis, direction, preferred_element_type=jnp.float32)
    return (update, new_one, new_two)
```

```python
import functools

import jax
import jax.numpy as jnp
from jax import lax
from jax.experimental import pallas as pl
from jax.experimental.pallas import tpu as pltpu
from jax.sharding import PartitionSpec as P

beta_one = 0.9
beta_two = 0.999
step_count = 10
epsilon = 1e-08


MESH = pl.DeviceIdType.MESH
LANES = 128
DEPTH = 4
f32, bf16 = jnp.float32, jnp.bfloat16


def kernel(
    R,
    C,
    K,
    q_hbm,
    g_hbm,
    m1_hbm,
    m2_hbm,
    up_hbm,
    n1_hbm,
    n2_hbm,
    qv,
    gT,
    pT,
    own,
    tmp,
    rsr,
    mT,
    dT,
    keep,
    give,
    pr,
    zr,
    zs,
    kz,
    stg,
    q_sem,
    stg_sem,
    out_sem,
    fin_sem,
    ag_send,
    ag_recv,
    rs_send,
    rs_recv,
    d_send,
    d_recv,
    pr_send,
    pr_recv,
    zs_sem,
    zr_sem,
    cred,
):
    Z = C // 2
    share = C // R
    rows_in, cols_in = qv.shape
    width = g_hbm.shape[1]
    p = width // K
    n_o = share * p
    N = C * p
    T1 = min(512, cols_in)
    T2 = min(512, rows_in)
    TR = stg.shape[1]
    LT = min(512, cols_in, rows_in)

    r = lax.axis_index("row")
    c = lax.axis_index("col")
    z = lax.div(c, 2)
    k = lax.rem(c, 2)
    partner = (r, z * 2 + 1 - k)
    above = (r, jnp.minimum(z + 1, Z - 1) * 2 + k)
    below = (r, jnp.maximum(z - 1, 0) * 2 + k)

    def peer(s):
        return (lax.rem(r + s, R), c)

    def al(x, m):
        return pl.multiple_of(x, m)

    def remote(src, dst, ss, rs, dev):
        return pltpu.make_async_remote_copy(
            src_ref=src, dst_ref=dst, send_sem=ss, recv_sem=rs, device_id=dev, device_id_type=MESH
        )

    barrier = pltpu.get_barrier_semaphore()

    def greet(dev):
        pl.semaphore_signal(barrier, inc=1, device_id=dev, device_id_type=MESH)

    for s in range(1, R):
        greet(peer(s))
    greet(partner)

    @pl.when(z < Z - 1)
    def _():
        greet(above)

    @pl.when(z > 0)
    def _():
        greet(below)

    q_copy = pltpu.make_async_copy(q_hbm, qv, q_sem)
    q_copy.start()

    def stream(src, j0, nj, ni, consume):
        n = nj * ni

        def fetch(i):
            return pltpu.make_async_copy(
                src.at[
                    pl.ds(al(lax.rem(i, ni) * TR, TR), TR), pl.ds(al((j0 + lax.div(i, ni)) * LANES, LANES), LANES)
                ],
                stg.at[lax.rem(i, DEPTH)],
                stg_sem.at[lax.rem(i, DEPTH)],
            )

        for i in range(min(DEPTH, n)):
            fetch(jnp.int32(i)).start()

        def body(i, carry):
            fetch(i).wait()
            consume(j0 + lax.div(i, ni), lax.rem(i, ni), jnp.transpose(stg[lax.rem(i, DEPTH)]))

            @pl.when(i + DEPTH < n)
            def _():
                fetch(i + DEPTH).start()

            return carry

        lax.fori_loop(0, n, body, 0)

    per_tile = LANES // p

    def take_gradient(j, i, x):
        x = x.astype(bf16)
        for s in range(per_tile):
            gT[j * per_tile + s, pl.ds(al(c * p, p), p), pl.ds(al(i * TR, TR), TR)] = x[s * p : (s + 1) * p, :]

    def take_moment(which):
        def take(j, i, x):
            mT[which, pl.ds(al(j * LANES, LANES), LANES), pl.ds(al(i * TR, TR), TR)] = x

        return take

    def block(ref, q, b):
        return ref.at[q, pl.ds(al(b * p, p), p), :]

    def ag_copy(way, q, zz):
        b = zz * 2 + k
        dev = (partner, above, below)[way]
        return remote(block(gT, q, b), block(gT, q, b), ag_send.at[way, q, zz], ag_recv.at[q, b], dev)

    def ag_own(q):
        @pl.when(z < Z - 1)
        def _():
            ag_copy(1, q, z).start()

        @pl.when(z > 0)
        def _():
            ag_copy(2, q, z).start()

        ag_copy(0, q, z).start()

    def ag_hop(q, h):
        @pl.when(z - h >= 0)
        def _():
            ag_copy(0, q, z - h).wait_recv()

            @pl.when(z < Z - 1)
            def _():
                ag_copy(1, q, z - h).start()

            ag_copy(0, q, z - h).start()

        @pl.when(z + h <= Z - 1)
        def _():
            ag_copy(0, q, z + h).wait_recv()

            @pl.when(z > 0)
            def _():
                ag_copy(2, q, z + h).start()

            ag_copy(0, q, z + h).start()

    def ag_wait(q):
        for zz in range(Z):
            b = zz * 2 + 1 - k
            remote(block(gT, q, b), block(gT, q, b), ag_send.at[0, q, zz], ag_recv.at[q, b], partner).wait_recv()

    def rs_copy(q, s):
        dst = lax.rem(r + s, R)
        return remote(
            pT.at[pl.ds(al(dst * n_o, n_o), n_o), :],
            rsr.at[lax.rem(q, 3), s - 1],
            rs_send.at[s - 1],
            rs_recv.at[lax.rem(q, 3), s - 1],
            peer(s),
        )

    def rotate(q):
        ag_wait(q)

        @pl.when(q > 0)
        def _():
            for s in range(1, R):
                rs_copy(q, s).wait_send()

        def body(j, carry):
            at = pl.ds(al(j * T1, T1), T1)
            tmp[:, :T1] = jnp.dot(gT[q], qv[:, at], preferred_element_type=f32)
            pT[:, at] = tmp[:, :T1].astype(bf16)
            own[lax.rem(q, 2), :, at] = tmp[pl.ds(al(r * n_o, n_o), n_o), :T1]
            return carry

        lax.fori_loop(0, cols_in // T1, body, 0)
        for s in range(1, R):
            rs_copy(q, s).start()

    def d_copy(q, s):
        mine = dT.at[lax.rem(q, 3), pl.ds(al(r * n_o, n_o), n_o), :]
        return remote(mine, mine, d_send.at[lax.rem(q, 2), s - 1], d_recv.at[lax.rem(q, 3), s - 1], peer(s))

    scale_one = 1.0 / (1.0 - beta_one**step_count)
    scale_two = 1.0 / (1.0 - beta_two**step_count)

    def adam(q):
        slot = lax.rem(q, 3)
        for s in range(1, R):
            rs_copy(q, s).wait_recv()
        for b in range(share):

            def body(j, carry):
                at = pl.ds(al(j * LT, LT), LT)
                rotated = own[lax.rem(q, 2), b * p : (b + 1) * p, at]
                if R <= 4:
                    for s in range(R - 1):
                        rotated = rotated + rsr[slot, s, b * p : (b + 1) * p, at].astype(f32)
                else:
                    rotated = lax.fori_loop(
                        0,
                        R - 1,
                        lambda s, acc: acc + rsr[slot, s, b * p : (b + 1) * p, at].astype(f32),
                        rotated,
                    )
                rows = pl.ds(al(b * width + q * p, p), p)
                new_one = beta_one * mT[0, rows, at] + (1.0 - beta_one) * rotated
                new_two = beta_two * mT[1, rows, at] + (1.0 - beta_two) * rotated * rotated
                mT[0, rows, at] = new_one
                mT[1, rows, at] = new_two
                direction = (new_one * scale_one) / (jnp.sqrt(new_two * scale_two) + epsilon)
                dT[slot, pl.ds(al(r * n_o + b * p, p), p), at] = direction.astype(bf16)
                return carry

            lax.fori_loop(0, cols_in // LT, body, 0)
        for s in range(1, R):
            d_copy(q, s).start()

        @pl.when(q == K - 1)
        def _():
            for w, out in enumerate((n1_hbm, n2_hbm)):
                pltpu.make_async_copy(mT.at[w], out, out_sem.at[w]).start()

    def pair_copy(q):
        return remote(give, pr.at[lax.rem(q, 2)], pr_send, pr_recv.at[lax.rem(q, 2)], partner)

    def back(q):
        slot = lax.rem(q, 3)
        for s in range(1, R):
            d_copy(q, s).wait_recv()

        @pl.when(q > 0)
        def _():
            pair_copy(q).wait_send()

        def body(j, carry):
            at = pl.ds(al(j * T2, T2), T2)
            tmp[:, :T2] = lax.dot_general(
                dT[slot], qv[at, :], (((1,), (1,)), ((), ())), preferred_element_type=f32
            )
            for g in range(Z):
                keep[g * p : (g + 1) * p, at] = tmp[pl.ds(al((2 * g + k) * p, p), p), :T2]
                give[g * p : (g + 1) * p, at] = tmp[pl.ds(al((2 * g + 1 - k) * p, p), p), :T2].astype(bf16)
            return carry

        lax.fori_loop(0, rows_in // T2, body, 0)
        pair_copy(q).start()
        for s in range(1, R):
            d_copy(q, s).wait_send()

    def fin_copy(q):
        return pltpu.make_async_copy(
            kz.at[lax.rem(q, 2)], up_hbm.at[pl.ds(al(q * p, p), p), :], fin_sem.at[lax.rem(q, 2)]
        )

    def tiles(fn):
        def body(j, carry):
            fn(pl.ds(al(j * LT, LT), LT))
            return carry

        lax.fori_loop(0, rows_in // LT, body, 0)

    def pair_sum(q):
        pair_copy(q).wait_recv()

        @pl.when(q >= 2)
        def _():
            fin_copy(q).wait()

        def add(at):
            for g in range(Z):
                rows = slice(g * p, (g + 1) * p)
                keep[rows, at] = keep[rows, at] + pr[lax.rem(q, 2), rows, at].astype(f32)
            kz[lax.rem(q, 2), :, at] = keep[pl.ds(al(z * p, p), p), at]

        tiles(add)

    def z_copy(q, g, up):
        s = lax.rem(q, 3)
        e = g + 1 if up else g
        return remote(zs.at[g], zr.at[s, e], zs_sem.at[g], zr_sem.at[s, e], above if up else below)

    def z_send(q, up, first):
        @pl.when(q >= 3)
        def _():
            pl.semaphore_wait(cred.at[0 if up else 1], 1)

        def one(i, carry):
            g = Z - 1 - i if up else i
            s = lax.rem(q, 3)
            e = g + 1 if up else g

            @pl.when(q > 0)
            def _():
                z_copy(q, g, up).wait_send()

            if not first:
                z_copy(q, g, up).wait_recv()

            def add(at):
                value = keep[pl.ds(al(g * p, p), p), at]
                if not first:
                    value = value + zr[s, e, :, at].astype(f32)
                zs[g, :, at] = value.astype(bf16)

            tiles(add)
            z_copy(q, g, up).start()
            return carry

        lax.fori_loop(0, Z - 1 - z if up else z, one, 0)

    def chain_ends(q):
        @pl.when(z == 0)
        def _():
            z_send(q, True, True)

        @pl.when(z == Z - 1)
        def _():
            z_send(q, False, True)

    def chain_near(q):
        @pl.when((z > 0) & (z < Z // 2))
        def _():
            z_send(q, True, False)

        @pl.when((z < Z - 1) & (z >= Z // 2))
        def _():
            z_send(q, False, False)

    def chain_far(q):
        @pl.when((z >= Z // 2) & (z < Z - 1))
        def _():
            z_send(q, True, False)

        @pl.when((z > 0) & (z < Z // 2))
        def _():
            z_send(q, False, False)

    def finish(q):
        s = lax.rem(q, 3)
        o = lax.rem(q, 2)

        @pl.when(z < Z - 1)
        def _():
            z_copy(q, z, False).wait_recv()

            def add(at):
                kz[o, :, at] = kz[o, :, at] + zr[s, z, :, at].astype(f32)

            tiles(add)

        @pl.when(z > 0)
        def _():
            z_copy(q, z, True).wait_recv()

            def add(at):
                kz[o, :, at] = kz[o, :, at] + zr[s, z + 1, :, at].astype(f32)

            tiles(add)

        fin_copy(q).start()

        @pl.when((q + 3 < K) & (z > 0))
        def _():
            pl.semaphore_signal(cred.at[0], inc=1, device_id=below, device_id_type=MESH)

        @pl.when((q + 3 < K) & (z < Z - 1))
        def _():
            pl.semaphore_signal(cred.at[1], inc=1, device_id=above, device_id_type=MESH)

    stream(g_hbm, 0, 1, rows_in // TR, take_gradient)
    pl.semaphore_wait(barrier, R + (z > 0).astype(jnp.int32) + (z < Z - 1).astype(jnp.int32))
    ag_own(0)
    ag_own(1)
    stream(m1_hbm, 0, share * width // LANES, cols_in // TR, take_moment(0))
    ag_hop(0, 1)
    if width > LANES:
        stream(g_hbm, 1, width // LANES - 1, rows_in // TR, take_gradient)
    for h in range(2, 2 + (Z - 2) // 2):
        ag_hop(0, h)
    stream(m2_hbm, 0, share * width // LANES, cols_in // TR, take_moment(1))
    for h in range(2 + (Z - 2) // 2, Z):
        ag_hop(0, h)
    q_copy.wait()

    hops = list(range(1, Z))
    third = -(-(Z - 1) // 3)
    groups = [hops[i * third : (i + 1) * third] for i in range(3)]

    def step(t, carry):
        def at_stage(lag, fn):
            q = t - lag

            @pl.when((q >= 0) & (q < K))
            def _():
                fn(q)

        def hop_group(i):
            def go(q):
                for h in groups[i]:
                    ag_hop(q, h)

            return go

        at_stage(-1, hop_group(0))
        at_stage(4, finish)
        at_stage(3, chain_near)
        at_stage(0, rotate)
        at_stage(-1, hop_group(1))
        at_stage(3, chain_far)
        at_stage(1, adam)
        at_stage(2, back)
        at_stage(-1, hop_group(2))
        at_stage(-2, ag_own)

        def pair(q):
            pair_sum(q)
            chain_ends(q)

        at_stage(2, pair)
        return carry

    lax.fori_loop(0, K + 4, step, 0)

    last = jnp.int32(K - 1)
    for s in range(1, R):
        rs_copy(last, s).wait_send()
    pair_copy(last).wait_send()
    for g in range(Z):

        @pl.when(z != g)
        def _():
            z_copy(last, g, True).wait_send()

    def drain(i, carry):
        q = lax.div(i, Z)
        zz = lax.rem(i, Z)
        ag_copy(0, q, zz).wait_send()

        @pl.when((zz <= z) & (z < Z - 1))
        def _():
            ag_copy(1, q, zz).wait_send()

        @pl.when((zz >= z) & (z > 0))
        def _():
            ag_copy(2, q, zz).wait_send()

        return carry

    lax.fori_loop(0, K * Z, drain, 0)
    fin_copy(last - 1).wait()
    fin_copy(last).wait()
    for w, out in enumerate((n1_hbm, n2_hbm)):
        pltpu.make_async_copy(mT.at[w], out, out_sem.at[w]).wait()


def local(R, C, eigenbasis, gradient, moment_one, moment_two):
    Z = C // 2
    share = C // R
    rows_in, cols_in = eigenbasis.shape
    width = gradient.shape[1]
    K = max(2, min(8, width // 16))
    p = width // K
    n_o = share * p
    N = C * p
    tile = min(512, rows_in, cols_in)
    dma = pltpu.SemaphoreType.DMA
    up, one, two = pl.pallas_call(
        functools.partial(kernel, R, C, K),
        out_shape=(
            jax.ShapeDtypeStruct((width, rows_in), f32),
            jax.ShapeDtypeStruct((share * width, cols_in), f32),
            jax.ShapeDtypeStruct((share * width, cols_in), f32),
        ),
        in_specs=[pl.BlockSpec(memory_space=pl.ANY)] * 4,
        out_specs=(pl.BlockSpec(memory_space=pl.ANY),) * 3,
        scratch_shapes=[
            pltpu.VMEM((rows_in, cols_in), bf16),
            pltpu.VMEM((K, N, rows_in), bf16),
            pltpu.VMEM((N, cols_in), bf16),
            pltpu.VMEM((2, n_o, cols_in), f32),
            pltpu.VMEM((N, 512), f32),
            pltpu.VMEM((3, R - 1, n_o, cols_in), bf16),
            pltpu.VMEM((2, share * width, cols_in), f32),
            pltpu.VMEM((3, N, cols_in), bf16),
            pltpu.VMEM((Z * p, rows_in), f32),
            pltpu.VMEM((Z * p, rows_in), bf16),
            pltpu.VMEM((2, Z * p, rows_in), bf16),
            pltpu.VMEM((3, Z + 1, p, rows_in), bf16),
            pltpu.VMEM((Z, p, rows_in), bf16),
            pltpu.VMEM((2, p, rows_in), f32),
            pltpu.VMEM((DEPTH, tile, LANES), f32),
            dma,
            dma((DEPTH,)),
            dma((2,)),
            dma((2,)),
            dma((3, K, Z)),
            dma((K, C)),
            dma((R - 1,)),
            dma((3, R - 1)),
            dma((2, R - 1)),
            dma((3, R - 1)),
            dma,
            dma((2,)),
            dma((Z,)),
            dma((3, Z + 1)),
            pltpu.SemaphoreType.REGULAR((2,)),
        ],
        compiler_params=pltpu.CompilerParams(
            collective_id=0, has_side_effects=True, vmem_limit_bytes=67043328
        ),
    )(eigenbasis, gradient, moment_one, moment_two)
    return up.T, one.T, two.T


def solution(mesh):
    rows, cols = mesh.shape["row"], mesh.shape["col"]
    return jax.shard_map(
        lambda *arrays: local(rows, cols, *arrays),
        mesh=mesh,
        in_specs=(P("row", "col"), P("row", "col"), P("col", "row"), P("col", "row")),
        out_specs=(P("row", "col"), P("col", "row"), P("col", "row")),
        check_vma=False,
    )
```

```python
import functools

import jax
import jax.numpy as jnp
from jax import lax
from jax.experimental import pallas as pl
from jax.experimental.pallas import tpu as pltpu
from jax.sharding import PartitionSpec as P

beta_one = 0.9
beta_two = 0.999
step_count = 10
epsilon = 1e-08


MESH = pl.DeviceIdType.MESH
LANES = 128
DEPTH = 4
f32, bf16 = jnp.float32, jnp.bfloat16


def kernel(
    R,
    C,
    K,
    q_hbm,
    g_hbm,
    m1_hbm,
    m2_hbm,
    up_hbm,
    n1_hbm,
    n2_hbm,
    qv,
    gT,
    pT,
    own,
    tmp,
    r1x,
    r1y,
    msx,
    msy,
    r2x,
    r2y,
    mT,
    dT,
    keep,
    give,
    pr,
    zr,
    zs,
    kz,
    stg,
    q_sem,
    stg_sem,
    out_sem,
    fin_sem,
    ag_send,
    ag_recv,
    r1_send,
    r1_recv,
    r2_send,
    r2_recv,
    d_send,
    d_recv,
    f_send,
    f_recv,
    pr_send,
    pr_recv,
    zs_sem,
    zr_sem,
    cred,
):
    Z = C // 2
    share = C // R
    rows_in, cols_in = qv.shape
    width = g_hbm.shape[1]
    p = width // K
    n_o = share * p
    N = C * p
    T1 = min(512, cols_in)
    T2 = min(512, rows_in)
    TR = stg.shape[1]
    H = cols_in // 2
    LT = min(512, H, rows_in)
    nx = max(d for d in range(1, R + 1) if R % d == 0 and d * d <= R)
    ny = R // nx

    r = lax.axis_index("row")
    c = lax.axis_index("col")
    z = lax.div(c, 2)
    k = lax.rem(c, 2)
    partner = (r, z * 2 + 1 - k)
    above = (r, jnp.minimum(z + 1, Z - 1) * 2 + k)
    below = (r, jnp.maximum(z - 1, 0) * 2 + k)

    y = lax.div(r, nx)
    x = lax.rem(r, nx)

    def row_of(yy, xx):
        return lax.rem(yy, ny) * nx + lax.rem(xx, nx)

    def al(x, m):
        return pl.multiple_of(x, m)

    def remote(src, dst, ss, rs, dev):
        return pltpu.make_async_remote_copy(
            src_ref=src, dst_ref=dst, send_sem=ss, recv_sem=rs, device_id=dev, device_id_type=MESH
        )

    barrier = pltpu.get_barrier_semaphore()

    def greet(dev):
        pl.semaphore_signal(barrier, inc=1, device_id=dev, device_id_type=MESH)

    for s in range(1, nx):
        greet((row_of(y, x + s), c))
    for s in range(1, ny):
        greet((row_of(y + s, x), c))
    greet(partner)

    @pl.when(z < Z - 1)
    def _():
        greet(above)

    @pl.when(z > 0)
    def _():
        greet(below)

    q_copy = pltpu.make_async_copy(q_hbm, qv, q_sem)
    q_copy.start()

    def stream(src, j0, nj, ni, consume):
        n = nj * ni

        def fetch(i):
            return pltpu.make_async_copy(
                src.at[
                    pl.ds(al(lax.rem(i, ni) * TR, TR), TR), pl.ds(al((j0 + lax.div(i, ni)) * LANES, LANES), LANES)
                ],
                stg.at[lax.rem(i, DEPTH)],
                stg_sem.at[lax.rem(i, DEPTH)],
            )

        for i in range(min(DEPTH, n)):
            fetch(jnp.int32(i)).start()

        def body(i, carry):
            fetch(i).wait()
            consume(j0 + lax.div(i, ni), lax.rem(i, ni), jnp.transpose(stg[lax.rem(i, DEPTH)]))

            @pl.when(i + DEPTH < n)
            def _():
                fetch(i + DEPTH).start()

            return carry

        lax.fori_loop(0, n, body, 0)

    per_tile = LANES // p

    def take_gradient(j, i, x):
        x = x.astype(bf16)
        for s in range(per_tile):
            gT[j * per_tile + s, pl.ds(al(c * p, p), p), pl.ds(al(i * TR, TR), TR)] = x[s * p : (s + 1) * p, :]

    def take_moment(which):
        def take(j, i, x):
            mT[which, pl.ds(al(j * LANES, LANES), LANES), pl.ds(al(i * TR, TR), TR)] = x

        return take

    def block(ref, q, b):
        return ref.at[q, pl.ds(al(b * p, p), p), :]

    def ag_copy(way, q, zz):
        b = zz * 2 + k
        dev = (partner, above, below)[way]
        return remote(block(gT, q, b), block(gT, q, b), ag_send.at[way, q, zz], ag_recv.at[q, b], dev)

    def ag_own(q):
        @pl.when(z < Z - 1)
        def _():
            ag_copy(1, q, z).start()

        @pl.when(z > 0)
        def _():
            ag_copy(2, q, z).start()

        ag_copy(0, q, z).start()

    def ag_hop(q, h):
        @pl.when(z - h >= 0)
        def _():
            ag_copy(0, q, z - h).wait_recv()

            @pl.when(z < Z - 1)
            def _():
                ag_copy(1, q, z - h).start()

            ag_copy(0, q, z - h).start()

        @pl.when(z + h <= Z - 1)
        def _():
            ag_copy(0, q, z + h).wait_recv()

            @pl.when(z > 0)
            def _():
                ag_copy(2, q, z + h).start()

            ag_copy(0, q, z + h).start()

    def ag_wait(q):
        for zz in range(Z):
            b = zz * 2 + 1 - k
            remote(block(gT, q, b), block(gT, q, b), ag_send.at[0, q, zz], ag_recv.at[q, b], partner).wait_recv()

    def part(ref, owner, lanes):
        return ref.at[pl.ds(al(owner * n_o, n_o), n_o), lanes]

    lower, upper = pl.ds(0, H), pl.ds(H, H)

    def r1_copies(q):
        o = lax.rem(q, 2)
        for s in range(1, ny):
            yy = lax.rem(y + s, ny)
            src = pT.at[pl.ds(al(yy * nx * n_o, nx * n_o), nx * n_o), lower]
            yield remote(src, r1y.at[o, s - 1], r1_send.at[0, s - 1, 0], r1_recv.at[o, 0, s - 1, 0], (row_of(yy, x), c))
        for s in range(1, nx):
            xx = lax.rem(x + s, nx)
            for yy in range(ny):
                yield remote(
                    part(pT, yy * nx + xx, upper),
                    r1x.at[o, s - 1, yy],
                    r1_send.at[1, s - 1, yy],
                    r1_recv.at[o, 1, s - 1, yy],
                    (row_of(y, xx), c),
                )

    def r2_copies(q):
        o = lax.rem(q, 2)
        for s in range(1, nx):
            yield remote(msx.at[s - 1], r2x.at[o, s - 1], r2_send.at[0, s - 1], r2_recv.at[o, 0, s - 1], (row_of(y, x + s), c))
        for s in range(1, ny):
            yield remote(msy.at[s - 1], r2y.at[o, s - 1], r2_send.at[1, s - 1], r2_recv.at[o, 1, s - 1], (row_of(y + s, x), c))

    def rotate(q):
        with jax.named_scope("rotate_wait"):
            ag_wait(q)

        @pl.when(q > 0)
        def _():
            for copy in r1_copies(q):
                copy.wait_send()

        def body(j, carry):
            at = pl.ds(al(j * T1, T1), T1)
            tmp[:, :T1] = jnp.dot(gT[q], qv[:, at], preferred_element_type=f32)
            pT[:, at] = tmp[:, :T1].astype(bf16)
            own[lax.rem(q, 2), :, at] = tmp[pl.ds(al(r * n_o, n_o), n_o), :T1]
            return carry

        lax.fori_loop(0, cols_in // T1, body, 0)
        for copy in r1_copies(q):
            copy.start()

    def middle(q):
        o = lax.rem(q, 2)
        with jax.named_scope("middle_wait"):
            for copy in r1_copies(q):
                copy.wait_recv()

        @pl.when(q > 0)
        def _():
            for copy in r2_copies(q):
                copy.wait_send()

        def body(j, carry):
            at = pl.ds(al(j * LT, LT), LT)
            hi = pl.ds(al(H + j * LT, LT), LT)

            def low(xx, value):
                for s in range(ny - 1):
                    value = value + r1y[o, s, pl.ds(al(xx * n_o, n_o), n_o), at].astype(f32)
                return value

            def high(yy, value):
                for s in range(nx - 1):
                    value = value + r1x[o, s, yy, :, at].astype(f32)
                return value

            own[o, :, at] = low(x, own[o, :, at])
            own[o, :, hi] = high(y, own[o, :, hi])
            for s in range(1, nx):
                xx = lax.rem(x + s, nx)
                rows = pl.ds(al((y * nx + xx) * n_o, n_o), n_o)
                msx[s - 1, :, at] = low(xx, pT[rows, at].astype(f32)).astype(bf16)
            for s in range(1, ny):
                yy = lax.rem(y + s, ny)
                rows = pl.ds(al((yy * nx + x) * n_o, n_o), n_o)
                msy[s - 1, :, at] = high(yy, pT[rows, hi].astype(f32)).astype(bf16)
            return carry

        lax.fori_loop(0, H // LT, body, 0)
        for copy in r2_copies(q):
            copy.start()

    def d_copies(q):
        o = lax.rem(q, 2)
        mine = dT.at[o, pl.ds(al(r * n_o, n_o), n_o), :]
        for s in range(1, nx):
            yield remote(mine, mine, d_send.at[o, 0, s - 1], d_recv.at[o, 0, s - 1], (row_of(y, x + s), c))
        for s in range(1, ny):
            yield remote(mine, mine, d_send.at[o, 1, s - 1], d_recv.at[o, 1, s - 1], (row_of(y + s, x), c))

    def d_waits(q):
        o = lax.rem(q, 2)

        def got(owner, sem, dev):
            rows = dT.at[o, pl.ds(al(owner * n_o, n_o), n_o), :]
            remote(rows, rows, d_send.at[o, 0, 0], sem, dev).wait_recv()

        for s in range(1, nx):
            got(row_of(y, x + nx - s), d_recv.at[o, 0, s - 1], (row_of(y, x + s), c))
        for s in range(1, ny):
            got(row_of(y + ny - s, x), d_recv.at[o, 1, s - 1], (row_of(y + s, x), c))

    def f_copies(q, arriving):
        o = lax.rem(q, 2)
        for a in range(1, nx):
            for b in range(1, ny):
                yy = y + ny - b if arriving else y
                piece = part(dT.at[o], row_of(yy, x + nx - a), lower)
                yield remote(piece, piece, f_send.at[o, 0, a - 1, b - 1], f_recv.at[o, 0, a - 1, b - 1], (row_of(y + b, x), c))
        for b in range(1, ny):
            for a in range(1, nx):
                xx = x + nx - a if arriving else x
                piece = part(dT.at[o], row_of(y + ny - b, xx), upper)
                yield remote(piece, piece, f_send.at[o, 1, a - 1, b - 1], f_recv.at[o, 1, a - 1, b - 1], (row_of(y, x + a), c))

    scale_one = 1.0 / (1.0 - beta_one**step_count)
    scale_two = 1.0 / (1.0 - beta_two**step_count)

    def adam(q):
        o = lax.rem(q, 2)
        with jax.named_scope("adam_wait"):
            for copy in r2_copies(q):
                copy.wait_recv()

        def one(b, half, j):
            at = pl.ds(al(j * LT, LT), LT)
            full = pl.ds(al(half * H + j * LT, LT), LT)
            mine = slice(b * p, (b + 1) * p)
            rotated = own[o, mine, full]
            ref, n = ((r2x, nx), (r2y, ny))[half]
            for s in range(n - 1):
                rotated = rotated + ref[o, s, mine, at].astype(f32)
            rows = pl.ds(al(b * width + q * p, p), p)
            new_one = beta_one * mT[0, rows, full] + (1.0 - beta_one) * rotated
            new_two = beta_two * mT[1, rows, full] + (1.0 - beta_two) * rotated * rotated
            mT[0, rows, full] = new_one
            mT[1, rows, full] = new_two
            direction = (new_one * scale_one) / (jnp.sqrt(new_two * scale_two) + epsilon)
            dT[o, pl.ds(al(r * n_o + b * p, p), p), full] = direction.astype(bf16)

        for b in range(share):
            for half in range(2):

                def body(j, carry):
                    one(b, half, j)
                    return carry

                lax.fori_loop(0, H // LT, body, 0)
        for copy in d_copies(q):
            copy.start()

        @pl.when(q == K - 1)
        def _():
            for w, out in enumerate((n1_hbm, n2_hbm)):
                pltpu.make_async_copy(mT.at[w], out, out_sem.at[w]).start()

    def forward(q):
        d_waits(q)
        for copy in f_copies(q, False):
            copy.start()

    def pair_copy(q):
        return remote(give, pr.at[lax.rem(q, 2)], pr_send, pr_recv.at[lax.rem(q, 2)], partner)

    def back(q):
        slot = lax.rem(q, 2)
        with jax.named_scope("back_wait"):
            for copy in f_copies(q, True):
                copy.wait_recv()

        @pl.when(q > 0)
        def _():
            pair_copy(q).wait_send()

        def body(j, carry):
            at = pl.ds(al(j * T2, T2), T2)
            tmp[:, :T2] = lax.dot_general(
                dT[slot], qv[at, :], (((1,), (1,)), ((), ())), preferred_element_type=f32
            )
            for g in range(Z):
                keep[slot, g * p : (g + 1) * p, at] = tmp[pl.ds(al((2 * g + k) * p, p), p), :T2]
                give[g * p : (g + 1) * p, at] = tmp[pl.ds(al((2 * g + 1 - k) * p, p), p), :T2].astype(bf16)
            return carry

        lax.fori_loop(0, rows_in // T2, body, 0)
        pair_copy(q).start()
        for copy in d_copies(q):
            copy.wait_send()
        for copy in f_copies(q, False):
            copy.wait_send()

    def fin_copy(q):
        return pltpu.make_async_copy(
            kz.at[lax.rem(q, 2)], up_hbm.at[pl.ds(al(q * p, p), p), :], fin_sem.at[lax.rem(q, 2)]
        )

    def tiles(fn):
        def body(j, carry):
            fn(pl.ds(al(j * LT, LT), LT))
            return carry

        lax.fori_loop(0, rows_in // LT, body, 0)

    def pair_sum(q):
        o = lax.rem(q, 2)
        with jax.named_scope("pair_wait"):
            pair_copy(q).wait_recv()

        @pl.when(q >= 2)
        def _():
            fin_copy(q).wait()

        def add(at):
            for g in range(Z):
                rows = slice(g * p, (g + 1) * p)
                keep[o, rows, at] = keep[o, rows, at] + pr[o, rows, at].astype(f32)
            kz[o, :, at] = keep[o, pl.ds(al(z * p, p), p), at]

        tiles(add)

    def z_copy(q, g, up):
        s = lax.rem(q, 3)
        e = g + 1 if up else g
        return remote(zs.at[g], zr.at[s, e], zs_sem.at[g], zr_sem.at[s, e], above if up else below)

    def z_send(q, up, first):
        @pl.when(q >= 3)
        def _():
            pl.semaphore_wait(cred.at[0 if up else 1], 1)

        def one(i, carry):
            g = Z - 1 - i if up else i
            s = lax.rem(q, 3)
            e = g + 1 if up else g

            @pl.when(q > 0)
            def _():
                z_copy(q, g, up).wait_send()

            if not first:
                z_copy(q, g, up).wait_recv()

            def add(at):
                value = keep[lax.rem(q, 2), pl.ds(al(g * p, p), p), at]
                if not first:
                    value = value + zr[s, e, :, at].astype(f32)
                zs[g, :, at] = value.astype(bf16)

            tiles(add)
            z_copy(q, g, up).start()
            return carry

        lax.fori_loop(0, Z - 1 - z if up else z, one, 0)

    def chain_ends(q):
        @pl.when(z == 0)
        def _():
            z_send(q, True, True)

        @pl.when(z == Z - 1)
        def _():
            z_send(q, False, True)

    def chain_near(q):
        @pl.when((z > 0) & (z < Z // 2))
        def _():
            z_send(q, True, False)

        @pl.when((z < Z - 1) & (z >= Z // 2))
        def _():
            z_send(q, False, False)

    def chain_far(q):
        @pl.when((z >= Z // 2) & (z < Z - 1))
        def _():
            z_send(q, True, False)

        @pl.when((z > 0) & (z < Z // 2))
        def _():
            z_send(q, False, False)

    def finish(q):
        s = lax.rem(q, 3)
        o = lax.rem(q, 2)

        @pl.when(z < Z - 1)
        def _():
            z_copy(q, z, False).wait_recv()

            def add(at):
                kz[o, :, at] = kz[o, :, at] + zr[s, z, :, at].astype(f32)

            tiles(add)

        @pl.when(z > 0)
        def _():
            z_copy(q, z, True).wait_recv()

            def add(at):
                kz[o, :, at] = kz[o, :, at] + zr[s, z + 1, :, at].astype(f32)

            tiles(add)

        fin_copy(q).start()

        @pl.when((q + 3 < K) & (z > 0))
        def _():
            pl.semaphore_signal(cred.at[0], inc=1, device_id=below, device_id_type=MESH)

        @pl.when((q + 3 < K) & (z < Z - 1))
        def _():
            pl.semaphore_signal(cred.at[1], inc=1, device_id=above, device_id_type=MESH)

    hops = list(range(1, Z))
    third = -(-(Z - 1) // 3)
    groups = [hops[i * third : (i + 1) * third] for i in range(3)]

    def hop_group(i):
        def go(q):
            for h in groups[i]:
                ag_hop(q, h)

        go.__name__ = f"hop{i}"
        return go

    with jax.named_scope("first_tile"):
        stream(g_hbm, 0, 1, rows_in // TR, take_gradient)
    with jax.named_scope("barrier"):
        pl.semaphore_wait(barrier, nx + ny - 1 + (z > 0).astype(jnp.int32) + (z < Z - 1).astype(jnp.int32))
    zero, one_ = jnp.int32(0), jnp.int32(1)
    ag_own(zero)
    with jax.named_scope("moment_one"):
        stream(m1_hbm, 0, share * width // LANES, cols_in // TR, take_moment(0))
    with jax.named_scope("hop_first"):
        hop_group(0)(zero)
    ag_own(one_)
    if width > LANES:
        with jax.named_scope("more_tiles"):
            stream(g_hbm, 1, width // LANES - 1, rows_in // TR, take_gradient)
    with jax.named_scope("hop_second"):
        hop_group(1)(zero)
        hop_group(0)(one_)
    with jax.named_scope("moment_two"):
        stream(m2_hbm, 0, share * width // LANES, cols_in // TR, take_moment(1))
    with jax.named_scope("hop_third"):
        hop_group(2)(zero)
        ag_own(jnp.int32(2))
        hop_group(1)(one_)
    q_copy.wait()

    def step(t, carry):
        def at_stage(lag, fn):
            q = t - lag

            @pl.when((q >= 0) & (q < K))
            def _():
                with jax.named_scope(fn.__name__):
                    fn(q)

        def pair(q):
            pair_sum(q)
            chain_ends(q)

        at_stage(1, adam)
        at_stage(0, rotate)
        at_stage(-2, hop_group(0))
        at_stage(1, forward)
        at_stage(4, finish)
        at_stage(3, chain_near)
        at_stage(2, back)
        at_stage(-3, ag_own)
        at_stage(-1, hop_group(2))
        at_stage(0, middle)
        at_stage(2, pair)
        at_stage(3, chain_far)
        at_stage(-2, hop_group(1))
        return carry

    lax.fori_loop(0, K + 4, step, 0)

    last = jnp.int32(K - 1)
    for copy in r1_copies(last):
        copy.wait_send()
    for copy in r2_copies(last):
        copy.wait_send()
    pair_copy(last).wait_send()
    for g in range(Z):

        @pl.when(z != g)
        def _():
            z_copy(last, g, True).wait_send()

    def drain(i, carry):
        q = lax.div(i, Z)
        zz = lax.rem(i, Z)
        ag_copy(0, q, zz).wait_send()

        @pl.when((zz <= z) & (z < Z - 1))
        def _():
            ag_copy(1, q, zz).wait_send()

        @pl.when((zz >= z) & (z > 0))
        def _():
            ag_copy(2, q, zz).wait_send()

        return carry

    lax.fori_loop(0, K * Z, drain, 0)
    fin_copy(last - 1).wait()
    fin_copy(last).wait()
    for w, out in enumerate((n1_hbm, n2_hbm)):
        pltpu.make_async_copy(mT.at[w], out, out_sem.at[w]).wait()


def local(R, C, eigenbasis, gradient, moment_one, moment_two):
    Z = C // 2
    share = C // R
    rows_in, cols_in = eigenbasis.shape
    width = gradient.shape[1]
    K = max(2, min(8, width // 16))
    p = width // K
    n_o = share * p
    N = C * p
    tile = min(512, rows_in, cols_in)
    half = cols_in // 2
    nx = max(d for d in range(1, R + 1) if R % d == 0 and d * d <= R)
    ny = R // nx
    most = max(nx, ny)
    dma = pltpu.SemaphoreType.DMA
    up, one, two = pl.pallas_call(
        functools.partial(kernel, R, C, K),
        out_shape=(
            jax.ShapeDtypeStruct((width, rows_in), f32),
            jax.ShapeDtypeStruct((share * width, cols_in), f32),
            jax.ShapeDtypeStruct((share * width, cols_in), f32),
        ),
        in_specs=[pl.BlockSpec(memory_space=pl.ANY)] * 4,
        out_specs=(pl.BlockSpec(memory_space=pl.ANY),) * 3,
        scratch_shapes=[
            pltpu.VMEM((rows_in, cols_in), bf16),
            pltpu.VMEM((K, N, rows_in), bf16),
            pltpu.VMEM((N, cols_in), bf16),
            pltpu.VMEM((2, n_o, cols_in), f32),
            pltpu.VMEM((N, 512), f32),
            pltpu.VMEM((2, nx - 1, ny, n_o, half), bf16),
            pltpu.VMEM((2, ny - 1, nx * n_o, half), bf16),
            pltpu.VMEM((nx - 1, n_o, half), bf16),
            pltpu.VMEM((ny - 1, n_o, half), bf16),
            pltpu.VMEM((2, nx - 1, n_o, half), bf16),
            pltpu.VMEM((2, ny - 1, n_o, half), bf16),
            pltpu.VMEM((2, share * width, cols_in), f32),
            pltpu.VMEM((2, N, cols_in), bf16),
            pltpu.VMEM((2, Z * p, rows_in), f32),
            pltpu.VMEM((Z * p, rows_in), bf16),
            pltpu.VMEM((2, Z * p, rows_in), bf16),
            pltpu.VMEM((3, Z + 1, p, rows_in), bf16),
            pltpu.VMEM((Z, p, rows_in), bf16),
            pltpu.VMEM((2, p, rows_in), f32),
            pltpu.VMEM((DEPTH, tile, LANES), f32),
            dma,
            dma((DEPTH,)),
            dma((2,)),
            dma((2,)),
            dma((3, K, Z)),
            dma((K, C)),
            dma((2, most, most)),
            dma((2, 2, most, most)),
            dma((2, most)),
            dma((2, 2, most)),
            dma((2, 2, most)),
            dma((2, 2, most)),
            dma((2, 2, most, most)),
            dma((2, 2, most, most)),
            dma,
            dma((2,)),
            dma((Z,)),
            dma((3, Z + 1)),
            pltpu.SemaphoreType.REGULAR((2,)),
        ],
        compiler_params=pltpu.CompilerParams(
            collective_id=0, has_side_effects=True, vmem_limit_bytes=67043328
        ),
    )(eigenbasis, gradient, moment_one, moment_two)
    parts = 8

    def flip(*refs):
        for src, dst in zip(refs[:3], refs[3:]):
            dst[...] = jnp.transpose(src[...])

    shapes = [(width, rows_in)] + [(share * width, cols_in)] * 2
    return pl.pallas_call(
        flip,
        grid=(parts,),
        out_shape=tuple(jax.ShapeDtypeStruct((b, a), f32) for a, b in shapes),
        in_specs=[pl.BlockSpec((a, b // parts), lambda i: (0, i)) for a, b in shapes],
        out_specs=tuple(pl.BlockSpec((b // parts, a), lambda i: (i, 0)) for a, b in shapes),
        compiler_params=pltpu.CompilerParams(dimension_semantics=("arbitrary",)),
    )(up, one, two)


def solution(mesh):
    rows, cols = mesh.shape["row"], mesh.shape["col"]
    return jax.shard_map(
        lambda *arrays: local(rows, cols, *arrays),
        mesh=mesh,
        in_specs=(P("row", "col"), P("row", "col"), P("col", "row"), P("col", "row")),
        out_specs=(P("row", "col"), P("col", "row"), P("col", "row")),
        check_vma=False,
    )
```

```python
import functools

import jax
import jax.numpy as jnp
from jax import lax
from jax.experimental import pallas as pl
from jax.experimental.pallas import tpu as pltpu
from jax.sharding import PartitionSpec as P

beta_one = 0.9
beta_two = 0.999
step_count = 10
epsilon = 1e-08


MESH = pl.DeviceIdType.MESH
LANES = 128
DEPTH = 4
f32, bf16 = jnp.float32, jnp.bfloat16


def kernel(
    R,
    C,
    K,
    q_hbm,
    g_hbm,
    m1_hbm,
    m2_hbm,
    up_hbm,
    n1_hbm,
    n2_hbm,
    qv,
    gT,
    pT,
    own,
    tmp,
    r1x,
    r1y,
    msx,
    msy,
    r2x,
    r2y,
    mT,
    dT,
    keep,
    give,
    pr,
    zr,
    zs,
    kz,
    stg,
    q_sem,
    stg_sem,
    out_sem,
    fin_sem,
    ag_send,
    ag_recv,
    r1_send,
    r1_recv,
    r2_send,
    r2_recv,
    d_send,
    d_recv,
    f_send,
    f_recv,
    pr_send,
    pr_recv,
    zs_sem,
    zr_sem,
    cred,
):
    Z = C // 2
    share = C // R
    rows_in, cols_in = qv.shape
    width = g_hbm.shape[1]
    p = width // K
    n_o = share * p
    N = C * p
    T1 = min(512, cols_in)
    T2 = min(512, rows_in)
    TR = stg.shape[1]
    H = cols_in // 2
    LT = min(512, H, rows_in)
    nx = max(d for d in range(1, R + 1) if R % d == 0 and d * d <= R)
    ny = R // nx

    r = lax.axis_index("row")
    c = lax.axis_index("col")
    z = lax.div(c, 2)
    k = lax.rem(c, 2)
    partner = (r, z * 2 + 1 - k)
    above = (r, jnp.minimum(z + 1, Z - 1) * 2 + k)
    below = (r, jnp.maximum(z - 1, 0) * 2 + k)

    y = lax.div(r, nx)
    x = lax.rem(r, nx)

    def row_of(yy, xx):
        return lax.rem(yy, ny) * nx + lax.rem(xx, nx)

    def al(x, m):
        return pl.multiple_of(x, m)

    def remote(src, dst, ss, rs, dev):
        return pltpu.make_async_remote_copy(
            src_ref=src, dst_ref=dst, send_sem=ss, recv_sem=rs, device_id=dev, device_id_type=MESH
        )

    barrier = pltpu.get_barrier_semaphore()

    def greet(dev):
        pl.semaphore_signal(barrier, inc=1, device_id=dev, device_id_type=MESH)

    for s in range(1, nx):
        greet((row_of(y, x + s), c))
    for s in range(1, ny):
        greet((row_of(y + s, x), c))
    greet(partner)

    @pl.when(z < Z - 1)
    def _():
        greet(above)

    @pl.when(z > 0)
    def _():
        greet(below)

    def stream(src, j0, nj, ni, consume):
        n = nj * ni

        def fetch(i):
            return pltpu.make_async_copy(
                src.at[
                    pl.ds(al(lax.rem(i, ni) * TR, TR), TR), pl.ds(al((j0 + lax.div(i, ni)) * LANES, LANES), LANES)
                ],
                stg.at[lax.rem(i, DEPTH)],
                stg_sem.at[lax.rem(i, DEPTH)],
            )

        for i in range(min(DEPTH, n)):
            fetch(jnp.int32(i)).start()

        def body(i, carry):
            fetch(i).wait()
            consume(j0 + lax.div(i, ni), lax.rem(i, ni), jnp.transpose(stg[lax.rem(i, DEPTH)]))

            @pl.when(i + DEPTH < n)
            def _():
                fetch(i + DEPTH).start()

            return carry

        lax.fori_loop(0, n, body, 0)

    per_tile = LANES // p

    def take_gradient(j, i, x):
        x = x.astype(bf16)
        for s in range(per_tile):
            gT[j * per_tile + s, pl.ds(al(c * p, p), p), pl.ds(al(i * TR, TR), TR)] = x[s * p : (s + 1) * p, :]

    def take_moment(which):
        def take(j, i, x):
            mT[which, pl.ds(al(j * LANES, LANES), LANES), pl.ds(al(i * TR, TR), TR)] = x

        return take

    def block(ref, q, b):
        return ref.at[q, pl.ds(al(b * p, p), p), :]

    def ag_copy(way, q, zz):
        b = zz * 2 + k
        dev = (partner, above, below)[way]
        return remote(block(gT, q, b), block(gT, q, b), ag_send.at[way, q, zz], ag_recv.at[q, b], dev)

    def ag_own(q):
        @pl.when(z < Z - 1)
        def _():
            ag_copy(1, q, z).start()

        @pl.when(z > 0)
        def _():
            ag_copy(2, q, z).start()

        ag_copy(0, q, z).start()

    def ag_hop(q, h):
        @pl.when(z - h >= 0)
        def _():
            ag_copy(0, q, z - h).wait_recv()

            @pl.when(z < Z - 1)
            def _():
                ag_copy(1, q, z - h).start()

            ag_copy(0, q, z - h).start()

        @pl.when(z + h <= Z - 1)
        def _():
            ag_copy(0, q, z + h).wait_recv()

            @pl.when(z > 0)
            def _():
                ag_copy(2, q, z + h).start()

            ag_copy(0, q, z + h).start()

    def ag_wait(q):
        for zz in range(Z):
            b = zz * 2 + 1 - k
            remote(block(gT, q, b), block(gT, q, b), ag_send.at[0, q, zz], ag_recv.at[q, b], partner).wait_recv()

    def part(ref, owner, lanes):
        return ref.at[pl.ds(al(owner * n_o, n_o), n_o), lanes]

    lower, upper = pl.ds(0, H), pl.ds(H, H)

    def r1_copies(q):
        o = lax.rem(q, 2)
        for s in range(1, ny):
            yy = lax.rem(y + s, ny)
            src = pT.at[pl.ds(al(yy * nx * n_o, nx * n_o), nx * n_o), lower]
            yield remote(src, r1y.at[o, s - 1], r1_send.at[0, s - 1, 0], r1_recv.at[o, 0, s - 1, 0], (row_of(yy, x), c))
        for s in range(1, nx):
            xx = lax.rem(x + s, nx)
            for yy in range(ny):
                yield remote(
                    part(pT, yy * nx + xx, upper),
                    r1x.at[o, s - 1, yy],
                    r1_send.at[1, s - 1, yy],
                    r1_recv.at[o, 1, s - 1, yy],
                    (row_of(y, xx), c),
                )

    def r2_copies(q):
        o = lax.rem(q, 2)
        for s in range(1, nx):
            yield remote(msx.at[s - 1], r2x.at[o, s - 1], r2_send.at[0, s - 1], r2_recv.at[o, 0, s - 1], (row_of(y, x + s), c))
        for s in range(1, ny):
            yield remote(msy.at[s - 1], r2y.at[o, s - 1], r2_send.at[1, s - 1], r2_recv.at[o, 1, s - 1], (row_of(y + s, x), c))

    def rotate(q):
        with jax.named_scope("rotate_wait"):
            ag_wait(q)

        @pl.when(q > 0)
        def _():
            for copy in r1_copies(q):
                copy.wait_send()

        def body(j, carry):
            at = pl.ds(al(j * T1, T1), T1)
            tmp[:, :T1] = jnp.dot(gT[q], qv[:, at], preferred_element_type=f32)
            pT[:, at] = tmp[:, :T1].astype(bf16)
            own[lax.rem(q, 2), :, at] = tmp[pl.ds(al(r * n_o, n_o), n_o), :T1]
            return carry

        lax.fori_loop(0, cols_in // T1, body, 0)

    def partials(q):
        for copy in r1_copies(q):
            copy.start()

    def middle(q):
        o = lax.rem(q, 2)
        with jax.named_scope("middle_wait"):
            for copy in r1_copies(q):
                copy.wait_recv()

        @pl.when(q > 0)
        def _():
            for copy in r2_copies(q):
                copy.wait_send()

        def body(j, carry):
            at = pl.ds(al(j * LT, LT), LT)
            hi = pl.ds(al(H + j * LT, LT), LT)

            def low(xx, value):
                for s in range(ny - 1):
                    value = value + r1y[o, s, pl.ds(al(xx * n_o, n_o), n_o), at].astype(f32)
                return value

            def high(yy, value):
                for s in range(nx - 1):
                    value = value + r1x[o, s, yy, :, at].astype(f32)
                return value

            own[o, :, at] = low(x, own[o, :, at])
            own[o, :, hi] = high(y, own[o, :, hi])
            for s in range(1, nx):
                xx = lax.rem(x + s, nx)
                rows = pl.ds(al((y * nx + xx) * n_o, n_o), n_o)
                msx[s - 1, :, at] = low(xx, pT[rows, at].astype(f32)).astype(bf16)
            for s in range(1, ny):
                yy = lax.rem(y + s, ny)
                rows = pl.ds(al((yy * nx + x) * n_o, n_o), n_o)
                msy[s - 1, :, at] = high(yy, pT[rows, hi].astype(f32)).astype(bf16)
            return carry

        lax.fori_loop(0, H // LT, body, 0)
        for copy in r2_copies(q):
            copy.start()

    def d_copies(q):
        o = lax.rem(q, 2)
        mine = dT.at[o, pl.ds(al(r * n_o, n_o), n_o), :]
        for s in range(1, nx):
            yield remote(mine, mine, d_send.at[o, 0, s - 1], d_recv.at[o, 0, s - 1], (row_of(y, x + s), c))
        for s in range(1, ny):
            yield remote(mine, mine, d_send.at[o, 1, s - 1], d_recv.at[o, 1, s - 1], (row_of(y + s, x), c))

    def d_waits(q):
        o = lax.rem(q, 2)

        def got(owner, sem, dev):
            rows = dT.at[o, pl.ds(al(owner * n_o, n_o), n_o), :]
            remote(rows, rows, d_send.at[o, 0, 0], sem, dev).wait_recv()

        for s in range(1, nx):
            got(row_of(y, x + nx - s), d_recv.at[o, 0, s - 1], (row_of(y, x + s), c))
        for s in range(1, ny):
            got(row_of(y + ny - s, x), d_recv.at[o, 1, s - 1], (row_of(y + s, x), c))

    def f_copies(q, arriving):
        o = lax.rem(q, 2)
        for a in range(1, nx):
            for b in range(1, ny):
                yy = y + ny - b if arriving else y
                piece = part(dT.at[o], row_of(yy, x + nx - a), lower)
                yield remote(piece, piece, f_send.at[o, 0, a - 1, b - 1], f_recv.at[o, 0, a - 1, b - 1], (row_of(y + b, x), c))
        for b in range(1, ny):
            for a in range(1, nx):
                xx = x + nx - a if arriving else x
                piece = part(dT.at[o], row_of(y + ny - b, xx), upper)
                yield remote(piece, piece, f_send.at[o, 1, a - 1, b - 1], f_recv.at[o, 1, a - 1, b - 1], (row_of(y, x + a), c))

    scale_one = 1.0 / (1.0 - beta_one**step_count)
    scale_two = 1.0 / (1.0 - beta_two**step_count)

    def adam(q):
        o = lax.rem(q, 2)
        with jax.named_scope("adam_wait"):
            for copy in r2_copies(q):
                copy.wait_recv()

        def one(b, half, j):
            at = pl.ds(al(j * LT, LT), LT)
            full = pl.ds(al(half * H + j * LT, LT), LT)
            mine = slice(b * p, (b + 1) * p)
            rotated = own[o, mine, full]
            ref, n = ((r2x, nx), (r2y, ny))[half]
            for s in range(n - 1):
                rotated = rotated + ref[o, s, mine, at].astype(f32)
            rows = pl.ds(al(b * width + q * p, p), p)
            new_one = beta_one * mT[0, rows, full] + (1.0 - beta_one) * rotated
            new_two = beta_two * mT[1, rows, full] + (1.0 - beta_two) * rotated * rotated
            mT[0, rows, full] = new_one
            mT[1, rows, full] = new_two
            direction = (new_one * scale_one) / (jnp.sqrt(new_two * scale_two) + epsilon)
            dT[o, pl.ds(al(r * n_o + b * p, p), p), full] = direction.astype(bf16)

        for b in range(share):
            for half in range(2):

                def body(j, carry):
                    one(b, half, j)
                    return carry

                lax.fori_loop(0, H // LT, body, 0)
        for copy in d_copies(q):
            copy.start()

        @pl.when(q == K - 1)
        def _():
            for w, out in enumerate((n1_hbm, n2_hbm)):
                pltpu.make_async_copy(mT.at[w], out, out_sem.at[w]).start()

    def forward(q):
        d_waits(q)
        for copy in f_copies(q, False):
            copy.start()

    def pair_copy(q):
        return remote(give, pr.at[lax.rem(q, 2)], pr_send, pr_recv.at[lax.rem(q, 2)], partner)

    def back(q):
        slot = lax.rem(q, 2)
        with jax.named_scope("back_wait"):
            for copy in f_copies(q, True):
                copy.wait_recv()

        @pl.when(q > 0)
        def _():
            pair_copy(q).wait_send()

        def body(j, carry):
            at = pl.ds(al(j * T2, T2), T2)
            tmp[:, :T2] = lax.dot_general(
                dT[slot], qv[at, :], (((1,), (1,)), ((), ())), preferred_element_type=f32
            )
            for g in range(Z):
                keep[slot, g * p : (g + 1) * p, at] = tmp[pl.ds(al((2 * g + k) * p, p), p), :T2]
                give[g * p : (g + 1) * p, at] = tmp[pl.ds(al((2 * g + 1 - k) * p, p), p), :T2].astype(bf16)
            return carry

        lax.fori_loop(0, rows_in // T2, body, 0)
        pair_copy(q).start()
        for copy in d_copies(q):
            copy.wait_send()
        for copy in f_copies(q, False):
            copy.wait_send()

    def fin_copy(q):
        return pltpu.make_async_copy(
            kz.at[lax.rem(q, 3)], up_hbm.at[pl.ds(al(q * p, p), p), :], fin_sem.at[lax.rem(q, 3)]
        )

    def tiles(fn):
        def body(j, carry):
            fn(pl.ds(al(j * LT, LT), LT))
            return carry

        lax.fori_loop(0, rows_in // LT, body, 0)

    def pair_sum(q):
        o = lax.rem(q, 2)
        with jax.named_scope("pair_wait"):
            pair_copy(q).wait_recv()

        @pl.when(q >= 3)
        def _():
            fin_copy(q).wait()

        def add(at):
            for g in range(Z):
                rows = slice(g * p, (g + 1) * p)
                keep[o, rows, at] = keep[o, rows, at] + pr[o, rows, at].astype(f32)
            kz[lax.rem(q, 3), :, at] = keep[o, pl.ds(al(z * p, p), p), at]

        tiles(add)

    def z_copy(q, g, up):
        s = lax.rem(q, 3)
        e = g + 1 if up else g
        return remote(zs.at[g], zr.at[s, e], zs_sem.at[g], zr_sem.at[s, e], above if up else below)

    def z_send(q, up, first):
        @pl.when(q >= 3)
        def _():
            pl.semaphore_wait(cred.at[0 if up else 1], 1)

        def one(i, carry):
            g = Z - 1 - i if up else i
            s = lax.rem(q, 3)
            e = g + 1 if up else g

            @pl.when(q > 0)
            def _():
                z_copy(q, g, up).wait_send()

            if not first:
                z_copy(q, g, up).wait_recv()

            def add(at):
                value = keep[lax.rem(q, 2), pl.ds(al(g * p, p), p), at]
                if not first:
                    value = value + zr[s, e, :, at].astype(f32)
                zs[g, :, at] = value.astype(bf16)

            tiles(add)
            z_copy(q, g, up).start()
            return carry

        lax.fori_loop(0, Z - 1 - z if up else z, one, 0)

    def chain_ends(q):
        @pl.when(z == 0)
        def _():
            z_send(q, True, True)

        @pl.when(z == Z - 1)
        def _():
            z_send(q, False, True)

    def chain_near(q):
        @pl.when((z > 0) & (z < Z // 2))
        def _():
            z_send(q, True, False)

        @pl.when((z < Z - 1) & (z >= Z // 2))
        def _():
            z_send(q, False, False)

    def chain_far(q):
        @pl.when((z >= Z // 2) & (z < Z - 1))
        def _():
            z_send(q, True, False)

        @pl.when((z > 0) & (z < Z // 2))
        def _():
            z_send(q, False, False)

    def finish(q):
        s = lax.rem(q, 3)
        o = s

        @pl.when(z < Z - 1)
        def _():
            z_copy(q, z, False).wait_recv()

            def add(at):
                kz[o, :, at] = kz[o, :, at] + zr[s, z, :, at].astype(f32)

            tiles(add)

        @pl.when(z > 0)
        def _():
            z_copy(q, z, True).wait_recv()

            def add(at):
                kz[o, :, at] = kz[o, :, at] + zr[s, z + 1, :, at].astype(f32)

            tiles(add)

        fin_copy(q).start()

        @pl.when((q + 3 < K) & (z > 0))
        def _():
            pl.semaphore_signal(cred.at[0], inc=1, device_id=below, device_id_type=MESH)

        @pl.when((q + 3 < K) & (z < Z - 1))
        def _():
            pl.semaphore_signal(cred.at[1], inc=1, device_id=above, device_id_type=MESH)

    hops = list(range(1, Z))
    third = -(-(Z - 1) // 3)
    groups = [hops[i * third : (i + 1) * third] for i in range(3)]

    def hop_group(i):
        def go(q):
            for h in groups[i]:
                ag_hop(q, h)

        go.__name__ = f"hop{i}"
        return go

    with jax.named_scope("first_tile"):
        stream(g_hbm, 0, 1, rows_in // TR, take_gradient)
    q_copy = pltpu.make_async_copy(q_hbm, qv, q_sem)
    q_copy.start()
    with jax.named_scope("barrier"):
        pl.semaphore_wait(barrier, nx + ny - 1 + (z > 0).astype(jnp.int32) + (z < Z - 1).astype(jnp.int32))
    zero, one_ = jnp.int32(0), jnp.int32(1)
    moment_tiles = share * width // LANES
    early = moment_tiles // 2
    ag_own(zero)
    with jax.named_scope("moment_one"):
        stream(m1_hbm, 0, moment_tiles, cols_in // TR, take_moment(0))
    with jax.named_scope("hop_first"):
        hop_group(0)(zero)
    if width > LANES:
        with jax.named_scope("more_tiles"):
            stream(g_hbm, 1, width // LANES - 1, rows_in // TR, take_gradient)
    if early:
        with jax.named_scope("moment_two"):
            stream(m2_hbm, 0, early, cols_in // TR, take_moment(1))
    with jax.named_scope("hop_second"):
        hop_group(1)(zero)
    ag_own(one_)
    with jax.named_scope("moment_two"):
        stream(m2_hbm, early, moment_tiles - early, cols_in // TR, take_moment(1))
    with jax.named_scope("hop_third"):
        hop_group(2)(zero)
    ag_own(jnp.int32(2))
    q_copy.wait()

    def step(t, carry):
        def at_stage(lag, fn):
            q = t - lag

            @pl.when((q >= 0) & (q < K))
            def _():
                with jax.named_scope(fn.__name__):
                    fn(q)

        def pair(q):
            pair_sum(q)
            chain_ends(q)

        at_stage(0, rotate)
        at_stage(0, partials)

        @pl.when(t == 0)
        def _():
            with jax.named_scope("hop_early"):
                hop_group(0)(one_)
                hop_group(1)(one_)

        at_stage(-2, hop_group(0))
        at_stage(2, back)
        at_stage(1, forward)
        at_stage(-3, ag_own)
        at_stage(-1, hop_group(2))
        at_stage(0, middle)
        at_stage(3, chain_near)
        at_stage(2, pair)
        at_stage(0, adam)
        at_stage(-2, hop_group(1))
        at_stage(3, chain_far)
        at_stage(4, finish)
        return carry

    lax.fori_loop(0, K + 4, step, 0)

    last = jnp.int32(K - 1)
    for copy in r1_copies(last):
        copy.wait_send()
    for copy in r2_copies(last):
        copy.wait_send()
    pair_copy(last).wait_send()
    for g in range(Z):

        @pl.when(z != g)
        def _():
            z_copy(last, g, True).wait_send()

    def drain(i, carry):
        q = lax.div(i, Z)
        zz = lax.rem(i, Z)
        ag_copy(0, q, zz).wait_send()

        @pl.when((zz <= z) & (z < Z - 1))
        def _():
            ag_copy(1, q, zz).wait_send()

        @pl.when((zz >= z) & (z > 0))
        def _():
            ag_copy(2, q, zz).wait_send()

        return carry

    lax.fori_loop(0, K * Z, drain, 0)
    for i in range(min(3, K)):
        fin_copy(last - i).wait()
    for w, out in enumerate((n1_hbm, n2_hbm)):
        pltpu.make_async_copy(mT.at[w], out, out_sem.at[w]).wait()


def local(R, C, eigenbasis, gradient, moment_one, moment_two):
    Z = C // 2
    share = C // R
    rows_in, cols_in = eigenbasis.shape
    width = gradient.shape[1]
    K = max(2, min(8, width // 16))
    p = width // K
    n_o = share * p
    N = C * p
    tile = min(512, rows_in, cols_in)
    half = cols_in // 2
    nx = max(d for d in range(1, R + 1) if R % d == 0 and d * d <= R)
    ny = R // nx
    most = max(nx, ny)
    dma = pltpu.SemaphoreType.DMA
    up, one, two = pl.pallas_call(
        functools.partial(kernel, R, C, K),
        out_shape=(
            jax.ShapeDtypeStruct((width, rows_in), f32),
            jax.ShapeDtypeStruct((share * width, cols_in), f32),
            jax.ShapeDtypeStruct((share * width, cols_in), f32),
        ),
        in_specs=[pl.BlockSpec(memory_space=pl.ANY)] * 4,
        out_specs=(pl.BlockSpec(memory_space=pl.ANY),) * 3,
        scratch_shapes=[
            pltpu.VMEM((rows_in, cols_in), bf16),
            pltpu.VMEM((K, N, rows_in), bf16),
            pltpu.VMEM((N, cols_in), bf16),
            pltpu.VMEM((2, n_o, cols_in), f32),
            pltpu.VMEM((N, 512), f32),
            pltpu.VMEM((2, nx - 1, ny, n_o, half), bf16),
            pltpu.VMEM((2, ny - 1, nx * n_o, half), bf16),
            pltpu.VMEM((nx - 1, n_o, half), bf16),
            pltpu.VMEM((ny - 1, n_o, half), bf16),
            pltpu.VMEM((2, nx - 1, n_o, half), bf16),
            pltpu.VMEM((2, ny - 1, n_o, half), bf16),
            pltpu.VMEM((2, share * width, cols_in), f32),
            pltpu.VMEM((2, N, cols_in), bf16),
            pltpu.VMEM((2, Z * p, rows_in), f32),
            pltpu.VMEM((Z * p, rows_in), bf16),
            pltpu.VMEM((2, Z * p, rows_in), bf16),
            pltpu.VMEM((3, Z + 1, p, rows_in), bf16),
            pltpu.VMEM((Z, p, rows_in), bf16),
            pltpu.VMEM((3, p, rows_in), f32),
            pltpu.VMEM((DEPTH, tile, LANES), f32),
            dma,
            dma((DEPTH,)),
            dma((2,)),
            dma((3,)),
            dma((3, K, Z)),
            dma((K, C)),
            dma((2, most, most)),
            dma((2, 2, most, most)),
            dma((2, most)),
            dma((2, 2, most)),
            dma((2, 2, most)),
            dma((2, 2, most)),
            dma((2, 2, most, most)),
            dma((2, 2, most, most)),
            dma,
            dma((2,)),
            dma((Z,)),
            dma((3, Z + 1)),
            pltpu.SemaphoreType.REGULAR((2,)),
        ],
        compiler_params=pltpu.CompilerParams(
            collective_id=0, has_side_effects=True, vmem_limit_bytes=67043328
        ),
    )(eigenbasis, gradient, moment_one, moment_two)
    parts = 8

    def flip(*refs):
        for src, dst in zip(refs[:3], refs[3:]):
            dst[...] = jnp.transpose(src[...])

    shapes = [(width, rows_in)] + [(share * width, cols_in)] * 2
    return pl.pallas_call(
        flip,
        grid=(parts,),
        out_shape=tuple(jax.ShapeDtypeStruct((b, a), f32) for a, b in shapes),
        in_specs=[pl.BlockSpec((a, b // parts), lambda i: (0, i)) for a, b in shapes],
        out_specs=tuple(pl.BlockSpec((b // parts, a), lambda i: (i, 0)) for a, b in shapes),
        compiler_params=pltpu.CompilerParams(dimension_semantics=("arbitrary",)),
    )(up, one, two)


def solution(mesh):
    rows, cols = mesh.shape["row"], mesh.shape["col"]
    return jax.shard_map(
        lambda *arrays: local(rows, cols, *arrays),
        mesh=mesh,
        in_specs=(P("row", "col"), P("row", "col"), P("col", "row"), P("col", "row")),
        out_specs=(P("row", "col"), P("col", "row"), P("col", "row")),
        check_vma=False,
    )
```

```python
import functools

import jax
import jax.numpy as jnp
from jax import lax
from jax.experimental import pallas as pl
from jax.experimental.pallas import tpu as pltpu
from jax.sharding import PartitionSpec as P

beta_one = 0.9
beta_two = 0.999
step_count = 10
epsilon = 1e-08


MESH = pl.DeviceIdType.MESH
LANES = 128
DEPTH = 4
f32, bf16 = jnp.float32, jnp.bfloat16


def kernel(
    R,
    C,
    K,
    q_hbm,
    g_hbm,
    m1_hbm,
    m2_hbm,
    up_hbm,
    n1_hbm,
    n2_hbm,
    qv,
    gT,
    pT,
    own,
    tmp,
    r1x,
    r1y,
    msx,
    msy,
    r2x,
    r2y,
    mT,
    dT,
    keep,
    give,
    pr,
    zr,
    zs,
    kz,
    stg,
    q_sem,
    stg_sem,
    out_sem,
    fin_sem,
    ag_send,
    ag_recv,
    r1_send,
    r1_recv,
    r2_send,
    r2_recv,
    d_send,
    d_recv,
    f_send,
    f_recv,
    pr_send,
    pr_recv,
    zs_sem,
    zr_sem,
    cred,
):
    Z = C // 2
    share = C // R
    rows_in, cols_in = qv.shape
    width = g_hbm.shape[1]
    p = width // K
    n_o = share * p
    N = C * p
    T1 = min(1024, cols_in)
    T2 = min(1024, rows_in)
    TR = stg.shape[1]
    H = cols_in // 2
    LT = min(512, H, rows_in)
    nx = max(d for d in range(1, R + 1) if R % d == 0 and d * d <= R)
    ny = R // nx

    r = lax.axis_index("row")
    c = lax.axis_index("col")
    z = lax.div(c, 2)
    k = lax.rem(c, 2)
    partner = (r, z * 2 + 1 - k)
    above = (r, jnp.minimum(z + 1, Z - 1) * 2 + k)
    below = (r, jnp.maximum(z - 1, 0) * 2 + k)

    y = lax.div(r, nx)
    x = lax.rem(r, nx)

    def row_of(yy, xx):
        return lax.rem(yy, ny) * nx + lax.rem(xx, nx)

    def al(x, m):
        return pl.multiple_of(x, m)

    def remote(src, dst, ss, rs, dev):
        return pltpu.make_async_remote_copy(
            src_ref=src, dst_ref=dst, send_sem=ss, recv_sem=rs, device_id=dev, device_id_type=MESH
        )

    barrier = pltpu.get_barrier_semaphore()

    def greet(dev):
        pl.semaphore_signal(barrier, inc=1, device_id=dev, device_id_type=MESH)

    for s in range(1, nx):
        greet((row_of(y, x + s), c))
    for s in range(1, ny):
        greet((row_of(y + s, x), c))
    greet(partner)

    @pl.when(z < Z - 1)
    def _():
        greet(above)

    @pl.when(z > 0)
    def _():
        greet(below)

    def stream(src, j0, nj, ni, consume):
        n = nj * ni

        def fetch(i):
            return pltpu.make_async_copy(
                src.at[
                    pl.ds(al(lax.rem(i, ni) * TR, TR), TR), pl.ds(al((j0 + lax.div(i, ni)) * LANES, LANES), LANES)
                ],
                stg.at[lax.rem(i, DEPTH)],
                stg_sem.at[lax.rem(i, DEPTH)],
            )

        for i in range(min(DEPTH, n)):
            fetch(jnp.int32(i)).start()

        def body(i, carry):
            fetch(i).wait()
            consume(j0 + lax.div(i, ni), lax.rem(i, ni), jnp.transpose(stg[lax.rem(i, DEPTH)]))

            @pl.when(i + DEPTH < n)
            def _():
                fetch(i + DEPTH).start()

            return carry

        lax.fori_loop(0, n, body, 0)

    per_tile = LANES // p

    def take_gradient(j, i, x):
        x = x.astype(bf16)
        for s in range(per_tile):
            gT[j * per_tile + s, pl.ds(al(c * p, p), p), pl.ds(al(i * TR, TR), TR)] = x[s * p : (s + 1) * p, :]

    def take_moment(which):
        def take(j, i, x):
            mT[which, pl.ds(al(j * LANES, LANES), LANES), pl.ds(al(i * TR, TR), TR)] = x

        return take

    def block(ref, q, b):
        return ref.at[q, pl.ds(al(b * p, p), p), :]

    def ag_copy(way, q, zz):
        b = zz * 2 + k
        dev = (partner, above, below)[way]
        return remote(block(gT, q, b), block(gT, q, b), ag_send.at[way, q, zz], ag_recv.at[q, b], dev)

    def ag_own(q):
        @pl.when(z < Z - 1)
        def _():
            ag_copy(1, q, z).start()

        @pl.when(z > 0)
        def _():
            ag_copy(2, q, z).start()

        ag_copy(0, q, z).start()

    def ag_hop(q, h):
        @pl.when(z - h >= 0)
        def _():
            ag_copy(0, q, z - h).wait_recv()

            @pl.when(z < Z - 1)
            def _():
                ag_copy(1, q, z - h).start()

            ag_copy(0, q, z - h).start()

        @pl.when(z + h <= Z - 1)
        def _():
            ag_copy(0, q, z + h).wait_recv()

            @pl.when(z > 0)
            def _():
                ag_copy(2, q, z + h).start()

            ag_copy(0, q, z + h).start()

    def ag_wait(q):
        for zz in range(Z):
            b = zz * 2 + 1 - k
            remote(block(gT, q, b), block(gT, q, b), ag_send.at[0, q, zz], ag_recv.at[q, b], partner).wait_recv()

    def part(ref, owner, lanes):
        return ref.at[pl.ds(al(owner * n_o, n_o), n_o), lanes]

    lower, upper = pl.ds(0, H), pl.ds(H, H)

    def r1_copies(q):
        o = lax.rem(q, 2)
        for s in range(1, ny):
            yy = lax.rem(y + s, ny)
            src = pT.at[pl.ds(al(yy * nx * n_o, nx * n_o), nx * n_o), lower]
            yield remote(src, r1y.at[o, s - 1], r1_send.at[0, s - 1, 0], r1_recv.at[o, 0, s - 1, 0], (row_of(yy, x), c))
        for s in range(1, nx):
            xx = lax.rem(x + s, nx)
            for yy in range(ny):
                yield remote(
                    part(pT, yy * nx + xx, upper),
                    r1x.at[o, s - 1, yy],
                    r1_send.at[1, s - 1, yy],
                    r1_recv.at[o, 1, s - 1, yy],
                    (row_of(y, xx), c),
                )

    def r2_copies(q):
        o = lax.rem(q, 2)
        for s in range(1, nx):
            yield remote(msx.at[s - 1], r2x.at[o, s - 1], r2_send.at[0, s - 1], r2_recv.at[o, 0, s - 1], (row_of(y, x + s), c))
        for s in range(1, ny):
            yield remote(msy.at[s - 1], r2y.at[o, s - 1], r2_send.at[1, s - 1], r2_recv.at[o, 1, s - 1], (row_of(y + s, x), c))

    def rotate(q):
        with jax.named_scope("rotate_wait"):
            ag_wait(q)

        @pl.when(q > 0)
        def _():
            for copy in r1_copies(q):
                copy.wait_send()

        def body(j, carry):
            at = pl.ds(al(j * T1, T1), T1)
            tmp[:, :T1] = jnp.dot(gT[q], qv[:, at], preferred_element_type=f32)
            pT[:, at] = tmp[:, :T1].astype(bf16)
            own[lax.rem(q, 2), :, at] = tmp[pl.ds(al(r * n_o, n_o), n_o), :T1]
            return carry

        lax.fori_loop(0, cols_in // T1, body, 0)

    def partials(q):
        for copy in r1_copies(q):
            copy.start()

    def middle(q):
        o = lax.rem(q, 2)
        with jax.named_scope("middle_wait"):
            for copy in r1_copies(q):
                copy.wait_recv()

        @pl.when(q > 0)
        def _():
            for copy in r2_copies(q):
                copy.wait_send()

        def body(j, carry):
            at = pl.ds(al(j * LT, LT), LT)
            hi = pl.ds(al(H + j * LT, LT), LT)

            def low(xx, value):
                for s in range(ny - 1):
                    value = value + r1y[o, s, pl.ds(al(xx * n_o, n_o), n_o), at].astype(f32)
                return value

            def high(yy, value):
                for s in range(nx - 1):
                    value = value + r1x[o, s, yy, :, at].astype(f32)
                return value

            own[o, :, at] = low(x, own[o, :, at])
            own[o, :, hi] = high(y, own[o, :, hi])
            for s in range(1, nx):
                xx = lax.rem(x + s, nx)
                rows = pl.ds(al((y * nx + xx) * n_o, n_o), n_o)
                msx[s - 1, :, at] = low(xx, pT[rows, at].astype(f32)).astype(bf16)
            for s in range(1, ny):
                yy = lax.rem(y + s, ny)
                rows = pl.ds(al((yy * nx + x) * n_o, n_o), n_o)
                msy[s - 1, :, at] = high(yy, pT[rows, hi].astype(f32)).astype(bf16)
            return carry

        lax.fori_loop(0, H // LT, body, 0)
        for copy in r2_copies(q):
            copy.start()

    def d_copies(q):
        o = lax.rem(q, 2)
        mine = dT.at[o, pl.ds(al(r * n_o, n_o), n_o), :]
        for s in range(1, nx):
            yield remote(mine, mine, d_send.at[o, 0, s - 1], d_recv.at[o, 0, s - 1], (row_of(y, x + s), c))
        for s in range(1, ny):
            yield remote(mine, mine, d_send.at[o, 1, s - 1], d_recv.at[o, 1, s - 1], (row_of(y + s, x), c))

    def d_waits(q):
        o = lax.rem(q, 2)

        def got(owner, sem, dev):
            rows = dT.at[o, pl.ds(al(owner * n_o, n_o), n_o), :]
            remote(rows, rows, d_send.at[o, 0, 0], sem, dev).wait_recv()

        for s in range(1, nx):
            got(row_of(y, x + nx - s), d_recv.at[o, 0, s - 1], (row_of(y, x + s), c))
        for s in range(1, ny):
            got(row_of(y + ny - s, x), d_recv.at[o, 1, s - 1], (row_of(y + s, x), c))

    def f_copies(q, arriving):
        o = lax.rem(q, 2)
        for a in range(1, nx):
            for b in range(1, ny):
                yy = y + ny - b if arriving else y
                piece = part(dT.at[o], row_of(yy, x + nx - a), lower)
                yield remote(piece, piece, f_send.at[o, 0, a - 1, b - 1], f_recv.at[o, 0, a - 1, b - 1], (row_of(y + b, x), c))
        for b in range(1, ny):
            for a in range(1, nx):
                xx = x + nx - a if arriving else x
                piece = part(dT.at[o], row_of(y + ny - b, xx), upper)
                yield remote(piece, piece, f_send.at[o, 1, a - 1, b - 1], f_recv.at[o, 1, a - 1, b - 1], (row_of(y, x + a), c))

    scale_one = 1.0 / (1.0 - beta_one**step_count)
    scale_two = 1.0 / (1.0 - beta_two**step_count)

    def adam(q):
        o = lax.rem(q, 2)
        with jax.named_scope("adam_wait"):
            for copy in r2_copies(q):
                copy.wait_recv()

        def one(b, half, j):
            at = pl.ds(al(j * LT, LT), LT)
            full = pl.ds(al(half * H + j * LT, LT), LT)
            mine = slice(b * p, (b + 1) * p)
            rotated = own[o, mine, full]
            ref, n = ((r2x, nx), (r2y, ny))[half]
            for s in range(n - 1):
                rotated = rotated + ref[o, s, mine, at].astype(f32)
            rows = pl.ds(al(b * width + q * p, p), p)
            new_one = beta_one * mT[0, rows, full] + (1.0 - beta_one) * rotated
            new_two = beta_two * mT[1, rows, full] + (1.0 - beta_two) * rotated * rotated
            mT[0, rows, full] = new_one
            mT[1, rows, full] = new_two
            direction = (new_one * scale_one) / (jnp.sqrt(new_two * scale_two) + epsilon)
            dT[o, pl.ds(al(r * n_o + b * p, p), p), full] = direction.astype(bf16)

        for b in range(share):
            for half in range(2):

                def body(j, carry):
                    one(b, half, j)
                    return carry

                lax.fori_loop(0, H // LT, body, 0)
        for copy in d_copies(q):
            copy.start()

        @pl.when(q == K - 1)
        def _():
            for w, out in enumerate((n1_hbm, n2_hbm)):
                pltpu.make_async_copy(mT.at[w], out, out_sem.at[w]).start()

    def forward(q):
        d_waits(q)
        for copy in f_copies(q, False):
            copy.start()

    def pair_copy(q):
        return remote(give, pr.at[lax.rem(q, 2)], pr_send, pr_recv.at[lax.rem(q, 2)], partner)

    def back(q):
        slot = lax.rem(q, 2)
        with jax.named_scope("back_wait"):
            for copy in f_copies(q, True):
                copy.wait_recv()

        @pl.when(q > 0)
        def _():
            pair_copy(q).wait_send()

        def body(j, carry):
            at = pl.ds(al(j * T2, T2), T2)
            tmp[:, :T2] = lax.dot_general(
                dT[slot], qv[at, :], (((1,), (1,)), ((), ())), preferred_element_type=f32
            )
            for g in range(Z):
                keep[slot, g * p : (g + 1) * p, at] = tmp[pl.ds(al((2 * g + k) * p, p), p), :T2]
                give[g * p : (g + 1) * p, at] = tmp[pl.ds(al((2 * g + 1 - k) * p, p), p), :T2].astype(bf16)
            return carry

        lax.fori_loop(0, rows_in // T2, body, 0)
        pair_copy(q).start()
        for copy in d_copies(q):
            copy.wait_send()
        for copy in f_copies(q, False):
            copy.wait_send()

    def fin_copy(q):
        return pltpu.make_async_copy(
            kz.at[lax.rem(q, 3)], up_hbm.at[pl.ds(al(q * p, p), p), :], fin_sem.at[lax.rem(q, 3)]
        )

    def tiles(fn):
        def body(j, carry):
            fn(pl.ds(al(j * LT, LT), LT))
            return carry

        lax.fori_loop(0, rows_in // LT, body, 0)

    def pair_sum(q):
        o = lax.rem(q, 2)
        with jax.named_scope("pair_wait"):
            pair_copy(q).wait_recv()

        @pl.when(q >= 3)
        def _():
            fin_copy(q).wait()

        def add(at):
            for g in range(Z):
                rows = slice(g * p, (g + 1) * p)
                keep[o, rows, at] = keep[o, rows, at] + pr[o, rows, at].astype(f32)
            kz[lax.rem(q, 3), :, at] = keep[o, pl.ds(al(z * p, p), p), at]

        tiles(add)

    def z_copy(q, g, up):
        s = lax.rem(q, 3)
        e = g + 1 if up else g
        o = lax.rem(q, 2)
        return remote(zs.at[o, g], zr.at[s, e], zs_sem.at[o, g], zr_sem.at[s, e], above if up else below)

    def z_send(q, up, first):
        @pl.when(q >= 3)
        def _():
            pl.semaphore_wait(cred.at[0 if up else 1], 1)

        def one(i, carry):
            g = Z - 1 - i if up else i
            s = lax.rem(q, 3)
            e = g + 1 if up else g

            @pl.when(q > 1)
            def _():
                z_copy(q, g, up).wait_send()

            if not first:
                z_copy(q, g, up).wait_recv()

            def add(at):
                value = keep[lax.rem(q, 2), pl.ds(al(g * p, p), p), at]
                if not first:
                    value = value + zr[s, e, :, at].astype(f32)
                zs[lax.rem(q, 2), g, :, at] = value.astype(bf16)

            tiles(add)
            z_copy(q, g, up).start()
            return carry

        lax.fori_loop(0, Z - 1 - z if up else z, one, 0)

    def chain_ends(q):
        @pl.when(z == 0)
        def _():
            z_send(q, True, True)

        @pl.when(z == Z - 1)
        def _():
            z_send(q, False, True)

    def chain_near(q):
        @pl.when((z > 0) & (z < Z // 2))
        def _():
            z_send(q, True, False)

        @pl.when((z < Z - 1) & (z >= Z // 2))
        def _():
            z_send(q, False, False)

    def chain_far(q):
        @pl.when((z >= Z // 2) & (z < Z - 1))
        def _():
            z_send(q, True, False)

        @pl.when((z > 0) & (z < Z // 2))
        def _():
            z_send(q, False, False)

    def finish(q):
        s = lax.rem(q, 3)
        o = s

        @pl.when(z < Z - 1)
        def _():
            z_copy(q, z, False).wait_recv()

            def add(at):
                kz[o, :, at] = kz[o, :, at] + zr[s, z, :, at].astype(f32)

            tiles(add)

        @pl.when(z > 0)
        def _():
            z_copy(q, z, True).wait_recv()

            def add(at):
                kz[o, :, at] = kz[o, :, at] + zr[s, z + 1, :, at].astype(f32)

            tiles(add)

        fin_copy(q).start()

        @pl.when((q + 3 < K) & (z > 0))
        def _():
            pl.semaphore_signal(cred.at[0], inc=1, device_id=below, device_id_type=MESH)

        @pl.when((q + 3 < K) & (z < Z - 1))
        def _():
            pl.semaphore_signal(cred.at[1], inc=1, device_id=above, device_id_type=MESH)

    hops = list(range(1, Z))
    third = -(-(Z - 1) // 3)
    groups = [hops[i * third : (i + 1) * third] for i in range(3)]

    def hop_group(i):
        def go(q):
            for h in groups[i]:
                ag_hop(q, h)

        go.__name__ = f"hop{i}"
        return go

    with jax.named_scope("first_tile"):
        stream(g_hbm, 0, 1, rows_in // TR, take_gradient)
    with jax.named_scope("barrier"):
        pl.semaphore_wait(barrier, nx + ny - 1 + (z > 0).astype(jnp.int32) + (z < Z - 1).astype(jnp.int32))
    zero, one_ = jnp.int32(0), jnp.int32(1)
    moment_tiles = share * width // LANES
    early = moment_tiles // 2
    ag_own(zero)
    with jax.named_scope("moment_one"):
        stream(m1_hbm, 0, moment_tiles, cols_in // TR, take_moment(0))
    q_copy = pltpu.make_async_copy(q_hbm, qv, q_sem)
    q_copy.start()
    with jax.named_scope("hop_first"):
        hop_group(0)(zero)
    if width > LANES:
        with jax.named_scope("more_tiles"):
            stream(g_hbm, 1, width // LANES - 1, rows_in // TR, take_gradient)
    if early:
        with jax.named_scope("moment_two"):
            stream(m2_hbm, 0, early, cols_in // TR, take_moment(1))
    with jax.named_scope("hop_second"):
        hop_group(1)(zero)
    ag_own(one_)
    with jax.named_scope("moment_two"):
        stream(m2_hbm, early, moment_tiles - early, cols_in // TR, take_moment(1))
    with jax.named_scope("hop_third"):
        hop_group(2)(zero)
    ag_own(jnp.int32(2))
    q_copy.wait()

    def step(t, carry):
        def at_stage(lag, fn):
            q = t - lag

            @pl.when((q >= 0) & (q < K))
            def _():
                with jax.named_scope(fn.__name__):
                    fn(q)

        def pair(q):
            pair_sum(q)
            chain_ends(q)

        at_stage(0, rotate)
        at_stage(0, partials)

        @pl.when(t == 0)
        def _():
            with jax.named_scope("hop_early"):
                hop_group(0)(one_)
                hop_group(1)(one_)

        at_stage(-2, hop_group(0))
        at_stage(2, back)
        at_stage(-3, ag_own)
        at_stage(-1, hop_group(2))
        at_stage(0, middle)
        at_stage(1, forward)
        at_stage(3, chain_near)
        at_stage(2, pair)
        at_stage(0, adam)
        at_stage(-2, hop_group(1))
        at_stage(3, chain_far)
        at_stage(4, finish)
        return carry

    lax.fori_loop(0, K + 4, step, 0)

    last = jnp.int32(K - 1)
    for copy in r1_copies(last):
        copy.wait_send()
    for copy in r2_copies(last):
        copy.wait_send()
    pair_copy(last).wait_send()
    for g in range(Z):

        @pl.when(z != g)
        def _():
            z_copy(last, g, True).wait_send()
            z_copy(last - 1, g, True).wait_send()

    def drain(i, carry):
        q = lax.div(i, Z)
        zz = lax.rem(i, Z)
        ag_copy(0, q, zz).wait_send()

        @pl.when((zz <= z) & (z < Z - 1))
        def _():
            ag_copy(1, q, zz).wait_send()

        @pl.when((zz >= z) & (z > 0))
        def _():
            ag_copy(2, q, zz).wait_send()

        return carry

    lax.fori_loop(0, K * Z, drain, 0)
    for i in range(min(3, K)):
        fin_copy(last - i).wait()
    for w, out in enumerate((n1_hbm, n2_hbm)):
        pltpu.make_async_copy(mT.at[w], out, out_sem.at[w]).wait()


def local(R, C, eigenbasis, gradient, moment_one, moment_two):
    Z = C // 2
    share = C // R
    rows_in, cols_in = eigenbasis.shape
    width = gradient.shape[1]
    K = max(2, min(8, width // 16))
    p = width // K
    n_o = share * p
    N = C * p
    tile = min(512, rows_in, cols_in)
    half = cols_in // 2
    nx = max(d for d in range(1, R + 1) if R % d == 0 and d * d <= R)
    ny = R // nx
    most = max(nx, ny)
    dma = pltpu.SemaphoreType.DMA
    up, one, two = pl.pallas_call(
        functools.partial(kernel, R, C, K),
        out_shape=(
            jax.ShapeDtypeStruct((width, rows_in), f32),
            jax.ShapeDtypeStruct((share * width, cols_in), f32),
            jax.ShapeDtypeStruct((share * width, cols_in), f32),
        ),
        in_specs=[pl.BlockSpec(memory_space=pl.ANY)] * 4,
        out_specs=(pl.BlockSpec(memory_space=pl.ANY),) * 3,
        scratch_shapes=[
            pltpu.VMEM((rows_in, cols_in), bf16),
            pltpu.VMEM((K, N, rows_in), bf16),
            pltpu.VMEM((N, cols_in), bf16),
            pltpu.VMEM((2, n_o, cols_in), f32),
            pltpu.VMEM((N, min(1024, max(rows_in, cols_in))), f32),
            pltpu.VMEM((2, nx - 1, ny, n_o, half), bf16),
            pltpu.VMEM((2, ny - 1, nx * n_o, half), bf16),
            pltpu.VMEM((nx - 1, n_o, half), bf16),
            pltpu.VMEM((ny - 1, n_o, half), bf16),
            pltpu.VMEM((2, nx - 1, n_o, half), bf16),
            pltpu.VMEM((2, ny - 1, n_o, half), bf16),
            pltpu.VMEM((2, share * width, cols_in), f32),
            pltpu.VMEM((2, N, cols_in), bf16),
            pltpu.VMEM((2, Z * p, rows_in), f32),
            pltpu.VMEM((Z * p, rows_in), bf16),
            pltpu.VMEM((2, Z * p, rows_in), bf16),
            pltpu.VMEM((3, Z + 1, p, rows_in), bf16),
            pltpu.VMEM((2, Z, p, rows_in), bf16),
            pltpu.VMEM((3, p, rows_in), f32),
            pltpu.VMEM((DEPTH, tile, LANES), f32),
            dma,
            dma((DEPTH,)),
            dma((2,)),
            dma((3,)),
            dma((3, K, Z)),
            dma((K, C)),
            dma((2, most, most)),
            dma((2, 2, most, most)),
            dma((2, most)),
            dma((2, 2, most)),
            dma((2, 2, most)),
            dma((2, 2, most)),
            dma((2, 2, most, most)),
            dma((2, 2, most, most)),
            dma,
            dma((2,)),
            dma((2, Z)),
            dma((3, Z + 1)),
            pltpu.SemaphoreType.REGULAR((2,)),
        ],
        compiler_params=pltpu.CompilerParams(
            collective_id=0, has_side_effects=True, vmem_limit_bytes=67043328
        ),
    )(eigenbasis, gradient, moment_one, moment_two)
    parts = 2

    def flip(*refs):
        for src, dst in zip(refs[:3], refs[3:]):
            dst[...] = jnp.transpose(src[...])

    shapes = [(width, rows_in)] + [(share * width, cols_in)] * 2
    return pl.pallas_call(
        flip,
        grid=(parts,),
        out_shape=tuple(jax.ShapeDtypeStruct((b, a), f32) for a, b in shapes),
        in_specs=[pl.BlockSpec((a, b // parts), lambda i: (0, i)) for a, b in shapes],
        out_specs=tuple(pl.BlockSpec((b // parts, a), lambda i: (i, 0)) for a, b in shapes),
        compiler_params=pltpu.CompilerParams(dimension_semantics=("arbitrary",)),
    )(up, one, two)


def solution(mesh):
    rows, cols = mesh.shape["row"], mesh.shape["col"]
    return jax.shard_map(
        lambda *arrays: local(rows, cols, *arrays),
        mesh=mesh,
        in_specs=(P("row", "col"), P("row", "col"), P("col", "row"), P("col", "row")),
        out_specs=(P("row", "col"), P("col", "row"), P("col", "row")),
        check_vma=False,
    )
```
